32 devices in a mesh: rep: 2 (over x), dp: 16 (over y, z, core).
Axes of the slice: x: 2, y: 2, z: 4, core: 2. Of those that a mesh axis runs over, the one named last changes fastest.
Arguments:
- x: bfloat16 [32, 2048, 768], P(('rep', 'dp')), parts along dimension 0
- dy: bfloat16 [32, 2048, 768], P(('rep', 'dp')), parts along dimension 0
- wq: bfloat16 [2, 768, 768], P(None, 'dp')
- wk: bfloat16 [2, 768, 768], P(None, 'dp')
- wv: bfloat16 [2, 768, 768], P(None, 'dp')
- wo: bfloat16 [2, 768, 768], P(None, 'dp')
- w_gate: bfloat16 [2, 768, 3072], P(None, 'dp')
- w_up: bfloat16 [2, 768, 3072], P(None, 'dp')
- w_down: bfloat16 [2, 3072, 768], P(None, 'dp')
Outputs:
- output 1: bfloat16 [32, 2048, 768], P(('rep', 'dp')), parts along dimension 0
- output 2: bfloat16 [4, 768, 768], P('rep', 'dp'), parts along dimension 0
- output 3: bfloat16 [4, 768, 768], P('rep', 'dp'), parts along dimension 0
- output 4: bfloat16 [4, 768, 768], P('rep', 'dp'), parts along dimension 0
- output 5: bfloat16 [4, 768, 768], P('rep', 'dp'), parts along dimension 0
- output 6: bfloat16 [4, 768, 3072], P('rep', 'dp'), parts along dimension 0
- output 7: bfloat16 [4, 768, 3072], P('rep', 'dp'), parts along dimension 0
- output 8: bfloat16 [4, 3072, 768], P('rep', 'dp'), parts along dimension 0
There are 2 independent parts. The reference program is written for one: setup_inputs(seed, part) draws one part's arguments, and reference() takes and returns one part's arrays. A program takes and returns all parts, laid end to end along the dimension named above; an argument that names none is the same for every part.
All inputs are finite; a program needn't handle non-finite values.
Results may differ from the reference program's by a relative error of at most 0.024.
Values are sent between devices in bfloat16 or wider.
A program may use at most 2 GiB of HBM per device.

```python
import jax
import jax.numpy as jnp
from jax import lax

SEQUENCES = 16
TOKENS = 2048
D = 768
HEADS = 6
KV_HEADS = 6
HEAD = 128
FF = 3072
LAYERS = 2
THETA = 10000
NAMES = ("wq", "wk", "wv", "wo", "w_gate", "w_up", "w_down")
SHAPES = {
    "wq": (LAYERS, D, HEADS * HEAD),
    "wk": (LAYERS, D, KV_HEADS * HEAD),
    "wv": (LAYERS, D, KV_HEADS * HEAD),
    "wo": (LAYERS, HEADS * HEAD, D),
    "w_gate": (LAYERS, D, FF),
    "w_up": (LAYERS, D, FF),
    "w_down": (LAYERS, FF, D),
}


def bump(key, n, height):
    away = (jnp.arange(n, dtype=jnp.int32) - jax.random.randint(key, (), 0, n, jnp.int32)) % n
    return jnp.where(away < n // 8, height, 1.0)


def together(key, own, strength):
    shared = jax.random.normal(key, own.shape[1:], jnp.float32)
    return (own + strength * shared) * lax.rsqrt(1 + strength * strength)


def setup_inputs(seed: int = 0, part: int = 0) -> dict:
    kx, kdy, ka, kb, kz, kf, kh, kl, *keys = jax.random.split(jax.random.key(seed), 8 + 3 * len(NAMES))
    kx, kdy, ka, kb = (jax.random.fold_in(k, part) for k in (kx, kdy, ka, kb))
    kw, km, kv = (keys[i::3] for i in range(3))
    shape = (SEQUENCES, TOKENS, D)
    much_x, much_dy = jax.random.uniform(kz, (2,), jnp.float32, 0.0, 1.0)
    loud = 2.0 ** jax.random.uniform(jax.random.fold_in(kz, 1), (), jnp.float32, -1.0, 2.0)
    layers = 2.0 ** jax.random.uniform(kl, (LAYERS, 1, 1), jnp.float32, -1.0, 1.0)
    times = {"wq": 1.0, "wk": 1.0, "wv": 2.0, "wo": layers, "w_gate": 1.0, "w_up": bump(kh, FF, 4.0), "w_down": layers}
    x = together(ka, jax.random.normal(kx, shape, jnp.float32), much_x) * bump(kf, D, 4.0)
    dy = together(kb, jax.random.normal(kdy, shape, jnp.float32), much_dy)
    drawn = {"x": x.astype(jnp.bfloat16), "dy": (loud * dy * (SEQUENCES * TOKENS) ** -0.5).astype(jnp.bfloat16)}
    for key, name in zip(kw, NAMES, strict=True):
        drawn[name] = (jax.random.normal(key, SHAPES[name], jnp.float32) * SHAPES[name][1] ** -0.5 * times[name]).astype(jnp.bfloat16)
    return drawn


def matmul(a, w):
    return jnp.dot(a, w, preferred_element_type=jnp.float32).astype(jnp.bfloat16)


def normed(h):
    wide = h.astype(jnp.float32)
    scale = lax.rsqrt(jnp.mean(wide**2, -1, keepdims=True) + 1e-6)
    return (wide * scale).astype(jnp.bfloat16)


def turned(t, theta):
    half = t.shape[-1] // 2
    angle = jnp.arange(t.shape[0], dtype=jnp.float32)[:, None] * theta ** (-jnp.arange(half, dtype=jnp.float32) / half)
    cos, sin = jnp.cos(angle)[:, None], jnp.sin(angle)[:, None]
    a, b = t[..., :half].astype(jnp.float32), t[..., half:].astype(jnp.float32)
    return jnp.concatenate([a * cos - b * sin, b * cos + a * sin], -1).astype(jnp.bfloat16)


def seen_by(q, k, v):
    tokens, kv = q.shape[0], k.shape[1]
    q = q.reshape(tokens, kv, -1, q.shape[-1])
    scores = jnp.einsum("tgsd,ugd->gstu", q.astype(jnp.float32), k.astype(jnp.float32)) * q.shape[-1] ** -0.5
    place = jnp.arange(tokens)
    weights = jax.nn.softmax(jnp.where(place[:, None] >= place, scores, -jnp.inf), -1).astype(jnp.bfloat16)
    return jnp.einsum("gstu,ugd->tgsd", weights.astype(jnp.float32), v.astype(jnp.float32)).astype(jnp.bfloat16).reshape(tokens, -1)


def layer(h, w):
    a = normed(h)
    q, k = (turned(matmul(a, w[name]).reshape(h.shape[0], -1, HEAD), THETA) for name in ("wq", "wk"))
    h = h + matmul(seen_by(q, k, matmul(a, w["wv"]).reshape(h.shape[0], -1, HEAD)), w["wo"])
    b = normed(h)
    gate = jnp.dot(b, w["w_gate"], preferred_element_type=jnp.float32)
    up = jnp.dot(b, w["w_up"], preferred_element_type=jnp.float32)
    return h + matmul((jax.nn.silu(gate) * up).astype(jnp.bfloat16), w["w_down"])


def stack(weights, h):
    return lax.scan(lambda h, w: (layer(h, w), None), h, weights)[0]


def reference(x, dy, wq, wk, wv, wo, w_gate, w_up, w_down):
    weights = dict(zip(NAMES, (wq, wk, wv, wo, w_gate, w_up, w_down), strict=True))

    def take(so_far, sequence):
        h, by_y = sequence
        _, back = jax.vjp(stack, weights, h)
        by_weights, by_h = back(by_y)
        return jax.tree.map(lambda total, term: total + term.astype(jnp.float32), so_far, by_weights), by_h

    none_yet = {name: jnp.zeros(w.shape, jnp.float32) for name, w in weights.items()}
    by_weights, by_x = lax.scan(take, none_yet, (x, dy))
    return (by_x, *(by_weights[name].astype(jnp.bfloat16) for name in NAMES))
```

```python
import functools

import jax
import jax.numpy as jnp
from jax import lax
from jax.experimental import pallas as pl
from jax.experimental.pallas import tpu as pltpu
from jax.experimental.layout import Layout, with_layout_constraint
from jax.sharding import PartitionSpec as P

NEG = -1e30
HIDDEN = 2 * NEG
LOG2E = 1.4426950408889634
VMEM = 56 * 2**20
HEAD = 128
THETA = 10000
BLOCK = 512
NAMES = ("wq", "wk", "wv", "wo", "w_gate", "w_up", "w_down")


def _dot(a, b, ca, cb):
    return lax.dot_general(a, b, (((ca,), (cb,)), ((), ())), preferred_element_type=jnp.float32)


def _turn(t, cos, sin):
    t = t.astype(jnp.float32)
    return (t * cos + pltpu.roll(t, HEAD // 2, 1) * sin).astype(jnp.bfloat16)


def _unturn(t, cos, sin):
    t = t.astype(jnp.float32)
    return (t * cos + pltpu.roll(t * sin, HEAD // 2, 1)).astype(jnp.bfloat16)


def _head(i):
    return slice(i * HEAD, (i + 1) * HEAD)


def _diagonal(n):
    return lax.broadcasted_iota(jnp.int32, (n, n), 1) >= lax.broadcasted_iota(jnp.int32, (n, n), 0)


def _forward(q_ref, k_ref, v_ref, cos_ref, sin_ref, o_ref, lse_ref, qr_ref, kr_ref, top_s, mix_s, *, scale, n):
    heads = q_ref.shape[1] // HEAD
    iq = pl.program_id(0)
    e = scale * LOG2E

    @pl.when(iq == 0)
    def _():
        @pl.loop(0, k_ref.shape[0] // n)
        def _(c):
            at = pl.ds(pl.multiple_of(c * n, n), n)
            for i in range(heads):
                kr_ref[at, _head(i)] = _turn(k_ref[at, _head(i)], cos_ref[at, :], sin_ref[at, :])

    mine = pl.ds(pl.multiple_of(iq * n, n), n)
    for i in range(heads):
        qr_ref[:, _head(i)] = _turn(q_ref[:, _head(i)], cos_ref[mine, :], sin_ref[mine, :])
        top_s[i : i + 1, :] = jnp.full((1, n), NEG, jnp.float32)
        mix_s[i] = jnp.zeros((HEAD + 8, n), jnp.float32)
    ones = jnp.ones((8, n), jnp.bfloat16)

    def block(j, masked):
        here = pl.ds(pl.multiple_of(j * n, n), n)
        scores = [_dot(kr_ref[here, _head(i)], qr_ref[:, _head(i)], 1, 1) for i in range(heads)]
        ok = _diagonal(n) if masked else None
        weights, keeps = [], []
        for i, s in enumerate(scores):
            if masked:
                s = jnp.where(ok, s, HIDDEN)
            old = top_s[i : i + 1, :]
            top = jnp.maximum(old, s.max(axis=0, keepdims=True))
            top_s[i : i + 1, :] = top
            weights.append(jnp.exp2((s - top) * e).astype(jnp.bfloat16))
            keeps.append(jnp.exp2((old - top) * e))
        for i, (p, keep) in enumerate(zip(weights, keeps)):
            values = jnp.concatenate([v_ref[here, _head(i)].T, ones], axis=0)
            mix_s[i] = mix_s[i] * keep + _dot(values, p, 1, 0)

    lax.fori_loop(0, iq, lambda j, _: block(j, False), None)
    block(iq, True)
    for i in range(heads):
        total = mix_s[i, HEAD : HEAD + 1, :]
        o_ref[:, _head(i)] = (mix_s[i, :HEAD, :] * (1 / total)).T.astype(o_ref.dtype)
        lse_ref[i] = top_s[i : i + 1, :] * scale + jnp.log(total)


def _backward(q_ref, k_ref, v_ref, do_ref, o_ref, lse_ref, cos_ref, sin_ref, dq_ref, dk_ref, dv_ref, dq_s, dk_s, dv_s, *, scale, n):
    heads = q_ref.shape[1] // HEAD
    iq = pl.program_id(1)
    e = scale * LOG2E

    @pl.when(iq == 0)
    def _():
        dk_s[...] = jnp.zeros_like(dk_s)
        dv_s[...] = jnp.zeros_like(dv_s)

    dq_s[...] = jnp.zeros_like(dq_s)
    mine = pl.ds(pl.multiple_of(iq * n, n), n)
    lses = [lse_ref[i] * LOG2E for i in range(heads)]
    deltas = [(do_ref[:, _head(i)].astype(jnp.float32) * o_ref[:, _head(i)].astype(jnp.float32)).T.sum(axis=0, keepdims=True) for i in range(heads)]

    def block(j, masked):
        here = pl.ds(pl.multiple_of(j * n, n), n)
        qs = [q_ref[:, _head(i)] for i in range(heads)]
        dos = [do_ref[:, _head(i)] for i in range(heads)]
        scores = [_dot(k_ref[here, _head(i)], qs[i], 1, 1) for i in range(heads)]
        dps = [_dot(v_ref[here, _head(i)], dos[i], 1, 1) for i in range(heads)]
        ok = _diagonal(n) if masked else None
        for i in range(heads):
            p = jnp.exp2(scores[i] * e - lses[i])
            if masked:
                p = jnp.where(ok, p, 0.0)
            ds = (p * (dps[i] - deltas[i])).astype(jnp.bfloat16)
            dv_s[i, here, :] += _dot(p.astype(jnp.bfloat16), dos[i], 1, 0)
            dk_s[i, here, :] += _dot(ds, qs[i], 1, 0)
            dq_s[i] += _dot(k_ref[here, _head(i)].T, ds, 1, 0)

    lax.fori_loop(0, iq, lambda j, _: block(j, False), None)
    block(iq, True)
    for i in range(heads):
        dq = (dq_s[i] * scale).T.astype(jnp.bfloat16)
        dq_ref[:, _head(i)] = _unturn(dq, cos_ref[mine, :], sin_ref[mine, :])

    @pl.when(iq == pl.num_programs(1) - 1)
    def _():
        @pl.loop(0, k_ref.shape[0] // n)
        def _(c):
            at = pl.ds(pl.multiple_of(c * n, n), n)
            for i in range(heads):
                dk = (dk_s[i, at, :] * scale).astype(jnp.bfloat16)
                dk_ref[at, _head(i)] = _unturn(dk, cos_ref[at, :], sin_ref[at, :])
                dv_ref[at, _head(i)] = dv_s[i, at, :].astype(jnp.bfloat16)


def _cost(tokens, width, matmuls, arrays):
    return pl.CostEstimate(flops=matmuls * tokens * tokens * width, transcendentals=tokens * tokens * width // (2 * HEAD), bytes_accessed=2 * arrays * tokens * width)


def attend(q, k, v, cos, sin):
    tokens, width = q.shape
    n, heads = min(BLOCK, tokens), width // HEAD
    some = pl.BlockSpec((n, width), lambda i: (i, 0))
    every = pl.BlockSpec((tokens, width), lambda i: (0, 0))
    table = pl.BlockSpec((tokens, HEAD), lambda i: (0, 0))
    like = jax.ShapeDtypeStruct((tokens, width), jnp.bfloat16)
    return pl.pallas_call(
        functools.partial(_forward, scale=HEAD**-0.5, n=n),
        grid=(tokens // n,),
        in_specs=[some, every, every, table, table],
        out_specs=[some, pl.BlockSpec((heads, 1, n), lambda i: (0, 0, i)), some, every],
        scratch_shapes=[pltpu.VMEM((heads, n), jnp.float32), pltpu.VMEM((heads, HEAD + 8, n), jnp.float32)],
        out_shape=[like, jax.ShapeDtypeStruct((heads, 1, tokens), jnp.float32), like, like],
        compiler_params=pltpu.CompilerParams(dimension_semantics=("arbitrary",), vmem_limit_bytes=VMEM),
        cost_estimate=_cost(tokens, width, 4, 6),
    )(q, k, v, cos, sin)


def attend_bwd(q, k, v, d_out, out, lse, cos, sin):
    tokens, width = q.shape
    n, heads = min(BLOCK, tokens), width // HEAD
    per = 3 if heads % 3 == 0 else 1
    some = pl.BlockSpec((n, per * HEAD), lambda g, i: (i, g))
    every = pl.BlockSpec((tokens, per * HEAD), lambda g, i: (0, g))
    table = pl.BlockSpec((tokens, HEAD), lambda g, i: (0, 0))
    like = jax.ShapeDtypeStruct((tokens, width), jnp.bfloat16)
    return pl.pallas_call(
        functools.partial(_backward, scale=HEAD**-0.5, n=n),
        grid=(heads // per, tokens // n),
        in_specs=[some, every, every, some, some, pl.BlockSpec((per, 1, n), lambda g, i: (g, 0, i)), table, table],
        out_specs=[some, every, every],
        scratch_shapes=[pltpu.VMEM((per, HEAD, n), jnp.float32), pltpu.VMEM((per, tokens, HEAD), jnp.float32), pltpu.VMEM((per, tokens, HEAD), jnp.float32)],
        out_shape=[like, like, like],
        compiler_params=pltpu.CompilerParams(dimension_semantics=("arbitrary", "arbitrary"), vmem_limit_bytes=VMEM),
        cost_estimate=_cost(tokens, width, 10, 8),
    )(q, k, v, d_out, out, lse, cos, sin)


@jax.custom_vjp
def attention(q, k, v, cos, sin):
    return attend(q, k, v, cos, sin)[0]


def _attention_fwd(q, k, v, cos, sin):
    out, lse, qr, kr = attend(q, k, v, cos, sin)
    return out, (qr, kr, v, out, lse, cos, sin)


def _attention_bwd(kept, d_out):
    qr, kr, v, out, lse, cos, sin = kept
    return (*attend_bwd(qr, kr, v, d_out, out, lse, cos, sin), None, None)


attention.defvjp(_attention_fwd, _attention_bwd)


def tables(tokens):
    half = HEAD // 2
    angle = jnp.arange(tokens, dtype=jnp.float32)[:, None] * THETA ** (-jnp.arange(half, dtype=jnp.float32) / half)
    cos, sin = jnp.cos(angle), jnp.sin(angle)
    return jnp.concatenate([cos, cos], -1), jnp.concatenate([-sin, sin], -1)


def matmul(a, w):
    return jnp.dot(a, w, preferred_element_type=jnp.float32).astype(jnp.bfloat16)


def normed(h):
    wide = h.astype(jnp.float32)
    scale = lax.rsqrt(jnp.mean(wide**2, -1, keepdims=True) + 1e-6)
    return (wide * scale).astype(jnp.bfloat16)


def attention_part(w, h, cos, sin):
    a = normed(h)
    q, k, v = (matmul(a, w[name]) for name in ("wq", "wk", "wv"))
    out = attention(q, k, v, cos, sin)
    return h + matmul(out, w["wo"]), out


def _chunks(tokens):
    n = min(BLOCK, tokens)
    return [slice(a, a + n) for a in range(0, tokens, n)]


def _mlp_up(b_ref, wg_ref, wu_ref, act_ref):
    for at in _chunks(b_ref.shape[0]):
        gate = _dot(b_ref[at, :], wg_ref[...], 1, 0)
        up = _dot(b_ref[at, :], wu_ref[...], 1, 0)
        act_ref[at, :] = (gate * jax.nn.sigmoid(gate) * up).astype(jnp.bfloat16)


def _mlp_grad(b_ref, dy_ref, wg_ref, wu_ref, wd_ref, dgate_ref, dup_ref, *act_ref):
    for at in _chunks(b_ref.shape[0]):
        gate = _dot(b_ref[at, :], wg_ref[...], 1, 0)
        up = _dot(b_ref[at, :], wu_ref[...], 1, 0)
        d_act = _dot(dy_ref[at, :], wd_ref[...], 1, 1).astype(jnp.bfloat16).astype(jnp.float32)
        sig = jax.nn.sigmoid(gate)
        silu = gate * sig
        if act_ref:
            act_ref[0][at, :] = (silu * up).astype(jnp.bfloat16)
        dup_ref[at, :] = (d_act * silu).astype(jnp.bfloat16)
        dgate_ref[at, :] = (d_act * up * (sig * (1 + gate * (1 - sig)))).astype(jnp.bfloat16)


def mlp_up(b, whole, gate_at, up_at, ff):
    tokens, d = b.shape
    n = min(BLOCK, ff)
    return pl.pallas_call(
        _mlp_up,
        grid=(ff // n,),
        in_specs=[pl.BlockSpec((tokens, d), lambda j: (0, 0)), pl.BlockSpec((d, n), lambda j: (0, gate_at // n + j)), pl.BlockSpec((d, n), lambda j: (0, up_at // n + j))],
        out_specs=pl.BlockSpec((tokens, n), lambda j: (0, j)),
        out_shape=jax.ShapeDtypeStruct((tokens, ff), jnp.bfloat16),
        compiler_params=pltpu.CompilerParams(dimension_semantics=("arbitrary",), vmem_limit_bytes=VMEM),
        cost_estimate=pl.CostEstimate(flops=4 * tokens * d * ff, transcendentals=tokens * ff, bytes_accessed=2 * tokens * (d + ff) + 4 * d * ff),
    )(b, whole, whole)


def mlp_grad(b, dy, whole, gate_at, up_at, w_down, with_act):
    tokens, d = b.shape
    ff = w_down.shape[0]
    n = min(BLOCK, ff)
    every, tile = pl.BlockSpec((tokens, d), lambda j: (0, 0)), pl.BlockSpec((tokens, n), lambda j: (0, j))
    outs = 3 if with_act else 2
    return pl.pallas_call(
        _mlp_grad,
        grid=(ff // n,),
        in_specs=[every, every, pl.BlockSpec((d, n), lambda j: (0, gate_at // n + j)), pl.BlockSpec((d, n), lambda j: (0, up_at // n + j)),
                  pl.BlockSpec((n, d), lambda j: (j, 0))],
        out_specs=[tile] * outs,
        out_shape=[jax.ShapeDtypeStruct((tokens, ff), jnp.bfloat16)] * outs,
        compiler_params=pltpu.CompilerParams(dimension_semantics=("arbitrary",), vmem_limit_bytes=VMEM),
        cost_estimate=pl.CostEstimate(flops=6 * tokens * d * ff, transcendentals=tokens * ff, bytes_accessed=2 * tokens * (2 * d + outs * ff) + 6 * d * ff),
    )(b, dy, whole, whole, w_down)


def _product(a, b, ca, cb):
    return _dot(a, b, ca, cb).astype(jnp.bfloat16)


def solution(mesh):
    size = mesh.shape["dp"]
    ATTN, MLP = NAMES[:4], NAMES[4:]

    def pieces(blocks, r):
        return [b[:, a : a + r, :] for b in blocks for a in range(0, b.shape[1], r)]

    def gather(parts, after):
        r = min(p.shape[0] for p in parts.values())
        packed = jnp.concatenate(pieces([p[None] for p in parts.values()], r), axis=2)[0]
        if after is not None:
            packed, after = lax.optimization_barrier((packed, after))
        return lax.all_gather(packed, "dp", axis=0, tiled=True), r

    def unpack(whole, r, parts):
        out, at = {}, 0
        for name, p in parts.items():
            rows, columns = p.shape
            n = rows // r
            if n == 1:
                out[name] = whole[:, at : at + columns]
            else:
                cut = [whole[:, at + i * columns : at + (i + 1) * columns].reshape(size, 1, r, columns) for i in range(n)]
                out[name] = jnp.concatenate(cut, axis=1).reshape(size * rows, columns)
            at += n * columns
        return out

    def pack(grads):
        grads = {name: with_layout_constraint(g, Layout(major_to_minor=(0, 1))) for name, g in grads.items()}
        blocks = {name: g.reshape(size, g.shape[0] // size, g.shape[1]) for name, g in grads.items()}
        r = min(b.shape[1] for b in blocks.values())
        packed = jnp.concatenate(pieces(list(blocks.values()), r), axis=2)
        return packed.reshape(size * r, packed.shape[2])

    def scatter(packed, grads, after):
        if after is not None:
            packed, after = lax.optimization_barrier((packed, after))
        got = lax.psum_scatter(packed, "dp", scatter_dimension=0, tiled=True)
        return unpacked(got, grads), got

    def unpacked(got, grads):
        r, out, at = got.shape[0], {}, 0
        for name, g in grads.items():
            rows, columns = g.shape[0] // size, g.shape[1]
            n = rows // r
            out[name] = jnp.concatenate([got[:, at + i * columns : at + (i + 1) * columns] for i in range(n)], axis=0)
            at += n * columns
        return out

    def halve(packed):
        me = lax.axis_index("dp")
        bits = size.bit_length() - 1
        left = list(reversed(range(bits)))
        sums = packed.reshape(*(2,) * bits, packed.shape[0] // size, packed.shape[1])
        for bit in [0, *reversed(range(1, bits))]:
            axis = left.index(bit)
            left.remove(bit)
            mine = lax.shift_right_logical(me, bit) & 1
            away = lax.dynamic_index_in_dim(sums, 1 - mine, axis, keepdims=False).astype(jnp.bfloat16)
            stays = lax.dynamic_index_in_dim(sums, mine, axis, keepdims=False)
            came = lax.ppermute(away, "dp", [(i, i ^ (1 << bit)) for i in range(size)])
            sums = stays.astype(jnp.float32) + came.astype(jnp.float32)
        return sums.astype(jnp.bfloat16)

    def step(x, dy, *weights):
        layers = weights[0].shape[0]
        own = dict(zip(NAMES, weights, strict=True))
        cos, sin = tables(x.shape[1])
        w, packs, places, whole = {}, [], [], None
        for number in range(layers):
            parts = {name: own[name][number] for name in NAMES}
            whole, r = gather(parts, whole)
            packs.append(whole)
            place, at = {}, 0
            for name, p in parts.items():
                place[name] = at
                at += p.size // r
            places.append(place)
            w.update({(number, name): m for name, m in unpack(whole, r, parts).items()})
        of = lambda number, names: {name: w[number, name] for name in names}
        h, back, kept, outs = x[0], {}, {}, {}
        ff = own["w_gate"].shape[2]
        for number in range(layers):
            h, back[number, "attn"], outs[number] = jax.vjp(lambda w, h: attention_part(w, h, cos, sin), of(number, ATTN), h, has_aux=True)
            b, back[number, "norm"] = jax.vjp(normed, h)
            act = None
            if number + 1 < layers:
                act = mlp_up(b, packs[number], places[number]["w_gate"], places[number]["w_up"], ff)
                h = h + matmul(act, w[number, "w_down"])
            kept[number] = b, act

        def mlp_back(number, by_h):
            b, act = kept[number]
            place = places[number]
            d_gate, d_up, *made = mlp_grad(b, by_h, packs[number], place["w_gate"], place["w_up"], w[number, "w_down"], act is None)
            act = made[0] if made else act
            by_b = _product(d_gate, w[number, "w_gate"], 1, 1) + _product(d_up, w[number, "w_up"], 1, 1)
            by_w = {"w_down": _product(act, by_h, 0, 0), "w_gate": _product(b, d_gate, 0, 0), "w_up": _product(b, d_up, 0, 0)}
            return by_w, by_h + back[number, "norm"](by_b)[0]

        by_h, mine, grads, got = dy[0], {}, {}, None
        for number in reversed(range(layers)):
            by_w, by_h = mlp_back(number, by_h)
            grads[number, "w_down"] = by_w["w_down"]
            cut, got = scatter(pack(grads), grads, got)
            mine.update(cut)
            grads = {(number, name): by_w[name] for name in ("w_gate", "w_up")}
            if number:
                packed, by_h = lax.optimization_barrier((pack(grads), by_h))
                cut, got = scatter(packed, grads, got)
                mine.update(cut)
                by_w, by_h = back[number, "attn"](by_h)
                grads = {(number, name): by_w[name] for name in ATTN}
        grads[0, "wo"] = _product(outs[0], by_h, 0, 0)
        packed, by_h = lax.optimization_barrier((pack(grads), by_h))
        cut, got = scatter(packed, grads, got)
        mine.update(cut)
        by_w, by_h = back[0, "attn"](by_h)
        grads = {(0, name): by_w[name] for name in ("wq", "wk", "wv")}
        mine.update(unpacked(halve(pack(grads)), grads))
        return (by_h[None], *(jnp.stack([mine[number, name] for number in range(layers)]) for name in NAMES))

    states, cut = P(("rep", "dp"), None, None), P(None, "dp", None)
    return jax.shard_map(
        step,
        mesh=mesh,
        in_specs=(states, states) + (cut,) * 7,
        out_specs=(states,) + (P("rep", "dp", None),) * 7,
        check_vma=False,
    )
```
